32 devices in a mesh: grp: 2 (over x), panel: 16 (over z, y, core).
Axes of the slice: x: 2, y: 2, z: 4, core: 2. Of those that a mesh axis runs over, the one named last changes fastest.
Arguments:
- density: bfloat16 [1024, 16, 128], P(('grp', 'panel')), parts along dimension 0, may hold values from -6 to 6
- near_blocks: bfloat16 [1024, 8, 128, 128], P(('grp', 'panel')), parts along dimension 0, may hold values from -0.1875 to 0.1875
- neighbours: int32 [1024, 8], P(('grp', 'panel')), parts along dimension 0, may hold values from 0 to 511, as said below
- counts: int32 [1024], P(('grp', 'panel')), parts along dimension 0, may hold values from 1 to 8, as said below
- coarse_map: int32 [1024], P(('grp', 'panel')), parts along dimension 0, may hold values from 0 to 31, as said below
- restrict: bfloat16 [1024, 128, 128], P(('grp', 'panel')), parts along dimension 0, may hold values from -0.125 to 0.125
- evaluate: bfloat16 [1024, 128, 128], P(('grp', 'panel')), parts along dimension 0, may hold values from -0.5 to 0.5
- coupling: float32 [64, 32], P(('grp', 'panel')), parts along dimension 0, as said below
Outputs:
- potential: bfloat16 [1024, 16, 128], P(('grp', 'panel')), parts along dimension 0
The draws below stay inside these ranges and needn't reach their ends.
There are 2 independent parts, one for each index of `grp`. The reference program is written for one: setup_inputs(seed, part) draws one part's arguments, and reference() takes and returns one part's arrays. A program takes and returns all parts, laid end to end along the dimension named above; each array names one. Nothing has to cross between parts.
Inputs may be any that keep to these rules, and one draw needn't show every extreme that they name: `neighbours`: slot 0 of block b is b itself; every entry lies within 16 blocks of b; in every draw some entry lies exactly 16 blocks below its block and some exactly 16 above. `counts`: every device holds blocks with all 8 slots live. `coarse_map`: block b's coarse cluster is one of the 2 clusters from (b // 32) * 2 on. `coupling`: the matrix is symmetric.
All inputs are finite; a program needn't handle non-finite values.
Results may differ from the reference program's by a relative error of at most 0.0042.
Values may be sent and summed in bfloat16 or wider, within the bound.
A program may use at most 64 MiB of HBM per device.

```python
import jax
import jax.numpy as jnp
from jax import lax

BLK = 128
RHS = 16
NB = 8
K = 128
COARSE_DEV = 2
BLK_DEV = 32
REACH = 16
NBLK = 512
NCOARSE = 32


def near_tables(key):
    key_offsets = jax.random.fold_in(key, 11)
    key_counts = jax.random.fold_in(key, 12)
    block_rows = jnp.arange(NBLK).astype(jnp.int32)
    offsets = jax.random.randint(key_offsets, (NBLK, NB), -REACH, REACH + 1).astype(jnp.int32)
    within = block_rows % BLK_DEV
    first_row = within == 0
    last_row = within == BLK_DEV - 1
    second = jnp.where(first_row, -REACH, jnp.where(last_row, REACH, offsets[:, 1])).astype(jnp.int32)
    offsets = offsets.at[:, 1].set(second)
    offsets = offsets.at[:, 0].set(0)
    block_ids = jnp.clip(block_rows[:, None] + offsets, 0, NBLK - 1).astype(jnp.int32)
    live_counts = jax.random.randint(key_counts, (NBLK,), 1, NB + 1).astype(jnp.int32)
    live_counts = jnp.where(first_row | last_row, NB, live_counts).astype(jnp.int32)
    return (block_ids, live_counts)


def draw_neighbours(key, part):
    return near_tables(key)[0]


def draw_counts(key, part):
    return near_tables(key)[1]


def draw_coarse_map(key, part):
    block_rows = jnp.arange(NBLK).astype(jnp.int32)
    chosen = jax.random.randint(jax.random.fold_in(key, 21), (NBLK,), 0, COARSE_DEV).astype(jnp.int32)
    return (block_rows // BLK_DEV * COARSE_DEV + chosen).astype(jnp.int32)


def draw_coupling(key, part):
    inner = jax.random.fold_in(key, 31)
    base = jax.random.normal(inner, (NCOARSE, NCOARSE), jnp.float32)
    return ((base + base.T) * (0.7071 / NCOARSE ** 0.5)).astype(jnp.float32)


def block_scale(rng, extent, split, smallest, top_value):
    def one(axis_at, blocks):
        steps = jax.random.uniform(jax.random.fold_in(jax.random.fold_in(rng, 6), axis_at), (blocks,), jnp.float32, smallest / len(split), top_value / len(split))
        return jnp.repeat(jnp.exp(steps), extent[axis_at] // blocks).reshape((-1,) + (1,) * (len(extent) - axis_at - 1))

    loudness = one(*split[0])
    for cut in split[1:]:
        loudness = loudness * one(*cut)
    return loudness


def noise(stream_key, dims, scale, reach, split=(), held_as=jnp.bfloat16):
    factor_of = block_scale(stream_key, dims, split, -0.22, 0.18) if split else 1.0
    result = jax.random.normal(stream_key, dims, jnp.float32) * scale * factor_of
    return jnp.minimum(jnp.maximum(result, -reach), reach).astype(held_as)


def setup_inputs(seed: int = 0, part: int = 0) -> dict:
    key_of = jax.random.split(jax.random.key(seed), 9)
    own_keys = jax.random.split(jax.random.fold_in(key_of[8], part), 9)
    density = noise(own_keys[0], (NBLK, RHS, BLK), 1.0, 6.0, ((0, 16),))
    near_blocks = noise(own_keys[1], (NBLK, NB, BLK, BLK), (BLK * NB) ** -0.5, 0.1875, ((0, 16),))
    neighbours = draw_neighbours(jax.random.fold_in(jax.random.fold_in(key_of[8], part), 71), part)
    counts = draw_counts(jax.random.fold_in(jax.random.fold_in(key_of[8], part), 71), part)
    coarse_map = draw_coarse_map(jax.random.fold_in(jax.random.fold_in(key_of[8], part), 71), part)
    restrict = noise(own_keys[5], (NBLK, K, BLK), (BLK * BLK_DEV // COARSE_DEV) ** -0.5, 0.125, ((0, 16),))
    evaluate = noise(own_keys[6], (NBLK, K, BLK), K ** -0.5, 0.5, ((0, 16),))
    coupling = draw_coupling(jax.random.fold_in(jax.random.fold_in(key_of[8], part), 71), part)
    return {"density": density, "near_blocks": near_blocks, "neighbours": neighbours, "counts": counts, "coarse_map": coarse_map, "restrict": restrict, "evaluate": evaluate, "coupling": coupling}


def reference(density, near_blocks, neighbours, counts, coarse_map, restrict, evaluate, coupling):
    dens_full = density.astype(jnp.float32)

    def one_block(item):
        blocks, block_ids, live_count = item
        picked = dens_full[block_ids]
        live_slots = (jnp.arange(NB).astype(jnp.int32) < live_count)[:, None, None]
        picked = jnp.where(live_slots, picked, jnp.zeros_like(picked))
        return jnp.einsum('jpq,jrq->rp', blocks.astype(jnp.float32), picked)

    near_part = lax.map(one_block, (near_blocks, neighbours, counts))
    block_terms = jnp.einsum('bkp,brp->brk', restrict.astype(jnp.float32), dens_full)
    block_terms = block_terms.reshape(NBLK, RHS * K)
    moments = jax.ops.segment_sum(block_terms, coarse_map, num_segments=NCOARSE)
    local_exp = jnp.dot(coupling, moments, precision=lax.Precision.HIGHEST).astype(jnp.bfloat16)
    spread = local_exp[coarse_map].astype(jnp.float32).reshape(NBLK, RHS, K)
    far_part = jnp.einsum('bkp,brk->brp', evaluate.astype(jnp.float32), spread)
    return (near_part + far_part).astype(jnp.bfloat16)
```

```python
import functools

import jax
import jax.numpy as jnp
from jax import lax
from jax.experimental import pallas as pl
from jax.experimental.pallas import tpu as pltpu
from jax.sharding import PartitionSpec as P

PARTS = 4
CONTRACT_LAST = (((1,), (1,)), ((), ()))


def kernel(count, dens_hbm, near_hbm, neigh_hbm, live_hbm, cmap_hbm, rest_hbm, eval_hbm, coup_hbm, out, neigh, live,
           cmap, coup, low, high, near, rest, evl, masked, moments, local_exp, acc, in_sem, rest_sem, near_sem, halo_send,
           halo_recv, send_sem, early_recv, late_recv, next_ready, ready, last_ready):
    slots, blk_count = neigh.shape
    reach = blk_count // 2
    columns = low.shape[1]
    coarse_dev = moments.shape[1]
    zero_slot = low.shape[0] - 1
    chips = count // 2
    last = chips - 1
    part = blk_count // PARTS
    me = lax.axis_index("panel")
    core = lax.rem(me, 2)
    chip = me // 2
    has_low = me > 0
    has_high = me < count - 1

    dens_copy = pltpu.make_async_copy(dens_hbm, low.at[pl.ds(reach, blk_count)], in_sem.at[0])
    high_copy = pltpu.make_async_copy(dens_hbm, high.at[pl.ds(0, blk_count)], in_sem.at[6])
    cmap_copy = pltpu.make_async_copy(cmap_hbm, cmap, in_sem.at[1])
    neigh_copy = pltpu.make_async_copy(neigh_hbm, neigh, in_sem.at[2])
    live_copy = pltpu.make_async_copy(live_hbm, live, in_sem.at[3])
    coup_copy = pltpu.make_async_copy(coup_hbm, coup, in_sem.at[4])
    eval_copy = pltpu.make_async_copy(eval_hbm, evl, in_sem.at[5])

    def rest_copy(i):
        blocks = pl.ds(i * part, part)
        return pltpu.make_async_copy(rest_hbm.at[blocks], rest.at[blocks], rest_sem.at[i])

    def near_copy(i):
        blocks = pl.ds(i * part, part)
        return pltpu.make_async_copy(near_hbm.at[blocks], near.at[blocks], near_sem.at[i])

    dens_copy.start()
    cmap_copy.start()
    for i in range(PARTS):
        rest_copy(i).start()
    high_copy.start()
    neigh_copy.start()
    live_copy.start()
    coup_copy.start()

    barrier = pltpu.get_barrier_semaphore()

    def greet(t, carry):
        pl.semaphore_signal(barrier, inc=1, device_id={"panel": t})
        return carry

    def answer(t, carry):
        pl.semaphore_signal(ready, inc=1, device_id={"panel": t})
        return carry

    def answer_last(t, carry):
        pl.semaphore_signal(last_ready, inc=1, device_id={"panel": t})
        return carry

    lax.fori_loop(me + 1, count, greet, 0)
    low[zero_slot] = jnp.zeros(low.shape[1:], low.dtype)
    high[zero_slot] = jnp.zeros(high.shape[1:], high.dtype)

    @pl.when(me == 0)
    def _():
        low[pl.ds(0, reach)] = jnp.zeros((reach,) + low.shape[1:], low.dtype)

    @pl.when(me == count - 1)
    def _():
        high[pl.ds(blk_count, reach)] = jnp.zeros((reach,) + high.shape[1:], high.dtype)

    @pl.when(has_low)
    def _():
        pl.semaphore_wait(barrier, me)
        pl.semaphore_signal(next_ready, inc=1, device_id={"panel": me - 1})

    @pl.when(chip < last)
    def _():
        lax.fori_loop(0, me, answer, 0)

    @pl.when(chip == last)
    def _():
        lax.fori_loop(0, me, answer_last, 0)

    dens_copy.wait()
    cmap_copy.wait()
    for b in range(blk_count):
        own = cmap[b] - me * coarse_dev
        values = low[reach + b].astype(jnp.float32)
        rows = [values * (own == c).astype(jnp.float32) for c in range(coarse_dev)]
        masked[b] = jnp.concatenate(rows, axis=0).astype(jnp.bfloat16)

    def halo(up):
        return pltpu.make_async_remote_copy(
            src_ref=low.at[pl.ds(blk_count if up else reach, reach)],
            dst_ref=low.at[pl.ds(0, reach)] if up else high.at[pl.ds(blk_count, reach)],
            send_sem=halo_send.at[int(up)], recv_sem=halo_recv.at[int(up)],
            device_id={"panel": me + 1 if up else me - 1})

    @pl.when(has_low & (chip < last))
    def _():
        halo(False).start()

    total = jnp.zeros((coarse_dev * columns, rest.shape[1]), jnp.float32)
    for i in range(PARTS):
        rest_copy(i).wait()
        if i == PARTS - 1:
            for k in range(PARTS):
                near_copy(lax.rem(k + (1 - core) * (PARTS // 2), PARTS)).start()
            eval_copy.start()
        blocks = range(i * part, (i + 1) * part)
        values = jnp.concatenate([masked[b] for b in blocks], axis=1)
        weights = jnp.concatenate([rest[b] for b in blocks], axis=1)
        total += lax.dot_general(values, weights, CONTRACT_LAST, preferred_element_type=jnp.float32)
    moments[me] = total.reshape(moments.shape[1:]).astype(jnp.bfloat16)

    def moment_copy(target, recv_sem):
        return pltpu.make_async_remote_copy(
            src_ref=moments.at[me], dst_ref=moments.at[me], send_sem=send_sem, recv_sem=recv_sem,
            device_id={"panel": target})

    def send(t, carry):
        moment_copy(t, early_recv).start()
        return carry

    def send_late(t, carry):
        moment_copy(t, late_recv).start()
        return carry

    @pl.when(chip < last)
    def _():
        lax.fori_loop(0, me, send, 0)

    @pl.when(chip == last)
    def _():
        lax.fori_loop(0, me, send_late, 0)

    @pl.when(chip == last)
    def _():
        halo(False).start()

    @pl.when(has_high)
    def _():
        pl.semaphore_wait(next_ready, 1)
        halo(True).start()

    @pl.when(me < count - 3)
    def _():
        pl.semaphore_wait(ready, count - 3 - me)
        lax.fori_loop(me + 1, count - 2, send, 0)

    @pl.when(chip < last)
    def _():
        pl.semaphore_wait(last_ready, 2)
        lax.fori_loop(count - 2, count, send, 0)

    @pl.when(me == count - 2)
    def _():
        pl.semaphore_wait(last_ready, 1)
        send_late(count - 1, 0)

    neigh_copy.wait()
    live_copy.wait()
    high_copy.wait()
    half = PARTS // 2

    def near_half(field, first, base):
        def near_part(i, carry):
            near_copy(first + i).wait()
            for t in range(part):
                b = (first + i) * part + t
                alive = live[b]
                places = [jnp.clip(neigh[j, b] - base, 0, zero_slot - 1) for j in range(slots)]
                picked = [field[jnp.where(j < alive, places[j], zero_slot)] for j in range(slots)]
                weights = jnp.concatenate([near[b, j] for j in range(slots)], axis=1)
                acc[b] = lax.dot_general(jnp.concatenate(picked, axis=1), weights, CONTRACT_LAST,
                                         preferred_element_type=jnp.float32)
            return carry

        lax.fori_loop(0, half, near_part, 0)

    def low_half():
        @pl.when(has_low)
        def _():
            halo(True).wait_recv()

        near_half(low, 0, me * blk_count - reach)

    def high_half():
        @pl.when(has_high)
        def _():
            halo(False).wait_recv()

        near_half(high, half, me * blk_count)

    @pl.when(core == 1)
    def _():
        low_half()
        high_half()

    @pl.when(core == 0)
    def _():
        high_half()
        low_half()

    def bytes_of(n, sem):
        block = moments.at[pl.ds(0, n)]
        return pltpu.make_async_copy(block, block, sem)

    coup_copy.wait()
    eval_copy.wait()

    @pl.when(chip < last)
    def _():
        bytes_of(count - 3, early_recv).wait()

    @pl.when(chip == last)
    def _():
        bytes_of(count - 2, early_recv).wait()

    sums = [jnp.zeros(moments.shape[2:], jnp.float32) for _ in range(coarse_dev)]

    def add(s):
        for i in range(coarse_dev):
            term = moments[s, i].astype(jnp.float32)
            for c in range(coarse_dev):
                sums[c] += coup[c, s * coarse_dev + i] * term

    for s in range(count - 2):
        add(s)

    @pl.when(chip < last)
    def _():
        bytes_of(2, late_recv).wait()

    @pl.when(chip == last)
    def _():
        bytes_of(1, late_recv).wait()

    add(count - 2)
    add(count - 1)
    for c in range(coarse_dev):
        local_exp[c] = sums[c].astype(jnp.bfloat16)

    for b in range(blk_count):
        spread = local_exp[jnp.clip(cmap[b] - me * coarse_dev, 0, coarse_dev - 1)]
        far = jnp.dot(spread, evl[b], preferred_element_type=jnp.float32)
        out[b] = (acc[b] + far).astype(jnp.bfloat16)

    @pl.when(has_high)
    def _():
        halo(True).wait_send()

    @pl.when(has_low)
    def _():
        halo(False).wait_send()

    bytes_of(count - 1, send_sem).wait()


def shards(count, density, near_blocks, neighbours, counts, coarse_map, restrict, evaluate, coupling):
    blk_count, columns, panels = density.shape
    terms = restrict.shape[1]
    coarse_dev = coupling.shape[0]
    hbm = pl.BlockSpec(memory_space=pl.ANY)
    dma = pltpu.SemaphoreType.DMA
    return pl.pallas_call(
        functools.partial(kernel, count),
        out_shape=pltpu.VMEM(density.shape, jnp.bfloat16),
        in_specs=[hbm] * 8,
        out_specs=pl.BlockSpec(memory_space=pltpu.VMEM),
        scratch_shapes=[
            pltpu.SMEM(neighbours.shape[::-1], jnp.int32),
            pltpu.SMEM(counts.shape, jnp.int32),
            pltpu.SMEM(coarse_map.shape, jnp.int32),
            pltpu.SMEM(coupling.shape, jnp.float32),
            pltpu.VMEM((blk_count + blk_count // 2 + 1, columns, panels), jnp.bfloat16),
            pltpu.VMEM((blk_count + blk_count // 2 + 1, columns, panels), jnp.bfloat16),
            pltpu.VMEM(near_blocks.shape, jnp.bfloat16),
            pltpu.VMEM(restrict.shape, jnp.bfloat16),
            pltpu.VMEM(evaluate.shape, jnp.bfloat16),
            pltpu.VMEM((blk_count, coarse_dev * columns, panels), jnp.bfloat16),
            pltpu.VMEM((count, coarse_dev, columns, terms), jnp.bfloat16),
            pltpu.VMEM((coarse_dev, columns, terms), jnp.bfloat16),
            pltpu.VMEM(density.shape, jnp.float32),
            dma((7,)),
            dma((PARTS,)),
            dma((PARTS,)),
            dma((2,)),
            dma((2,)),
            dma,
            dma,
            dma,
            pltpu.SemaphoreType.REGULAR,
            pltpu.SemaphoreType.REGULAR,
            pltpu.SemaphoreType.REGULAR,
        ],
        compiler_params=pltpu.CompilerParams(collective_id=0, has_side_effects=True),
    )(density, near_blocks, neighbours.T, counts, coarse_map, restrict, evaluate, coupling)


def solution(mesh):
    rows = ("grp", "panel")
    placed = (
        P(rows, None, None),
        P(rows, None, None, None),
        P(rows, None),
        P(rows),
        P(rows),
        P(rows, None, None),
        P(rows, None, None),
        P(rows, None),
    )
    return jax.shard_map(
        functools.partial(shards, mesh.shape["panel"]),
        mesh=mesh,
        in_specs=placed,
        out_specs=P(rows, None, None),
        check_vma=False,
    )
```

```python
import functools

import jax
import jax.numpy as jnp
from jax import lax
from jax.experimental import pallas as pl
from jax.experimental.pallas import tpu as pltpu
from jax.sharding import PartitionSpec as P

PARTS = 4
CONTRACT_LAST = (((1,), (1,)), ((), ()))


def kernel(count, dens_hbm, near_hbm, neigh_hbm, live_hbm, cmap_hbm, rest_hbm, eval_hbm, coup_hbm, out, neigh, live,
           cmap, coup, low, high, near, rest, evl, masked, moments, acc, halo_recv, early_recv, late_recv, next_ready, ready, last_ready):
    slots, blk_count = neigh.shape
    reach = blk_count // 2
    columns, panels = low.shape[1:]
    coarse_dev = moments.shape[1]
    zero_slot = low.shape[0] - 1
    chips = count // 2
    last = chips - 1
    part = blk_count // PARTS
    me = lax.axis_index("panel")
    core = lax.rem(me, 2)
    chip = me // 2
    has_low = me > 0
    has_high = me < count - 1

    def bytes_of(n, sem):
        block = moments.at[pl.ds(0, n)]
        return pltpu.make_async_copy(block, block, sem)

    def gather(in_sem, rest_sem, near_sem, halo_send, send_sem):
        dens_copy = pltpu.make_async_copy(dens_hbm, low.at[pl.ds(reach, blk_count)], in_sem.at[0])
        high_copy = pltpu.make_async_copy(dens_hbm, high.at[pl.ds(0, blk_count)], in_sem.at[6])
        cmap_copy = pltpu.make_async_copy(cmap_hbm, cmap, in_sem.at[1])
        neigh_copy = pltpu.make_async_copy(neigh_hbm, neigh, in_sem.at[2])
        live_copy = pltpu.make_async_copy(live_hbm, live, in_sem.at[3])
        coup_copy = pltpu.make_async_copy(coup_hbm, coup, in_sem.at[4])
        eval_copy = pltpu.make_async_copy(eval_hbm, evl, in_sem.at[5])

        def rest_copy(i):
            blocks = pl.ds(i * part, part)
            return pltpu.make_async_copy(rest_hbm.at[blocks], rest.at[blocks], rest_sem.at[i])

        def near_copy(i):
            blocks = pl.ds(i * part, part)
            return pltpu.make_async_copy(near_hbm.at[blocks], near.at[blocks], near_sem.at[i])

        dens_copy.start()
        cmap_copy.start()
        for i in range(PARTS):
            rest_copy(i).start()
        high_copy.start()
        neigh_copy.start()
        live_copy.start()
        coup_copy.start()

        barrier = pltpu.get_barrier_semaphore()

        def greet(t, carry):
            pl.semaphore_signal(barrier, inc=1, device_id={"panel": t})
            return carry

        def answer(t, carry):
            pl.semaphore_signal(ready, inc=1, device_id={"panel": t})
            return carry

        def answer_last(t, carry):
            pl.semaphore_signal(last_ready, inc=1, device_id={"panel": t})
            return carry

        lax.fori_loop(me + 1, count, greet, 0)
        low[zero_slot] = jnp.zeros(low.shape[1:], low.dtype)
        high[zero_slot] = jnp.zeros(high.shape[1:], high.dtype)

        @pl.when(me == 0)
        def _():
            low[pl.ds(0, reach)] = jnp.zeros((reach,) + low.shape[1:], low.dtype)

        @pl.when(me == count - 1)
        def _():
            high[pl.ds(blk_count, reach)] = jnp.zeros((reach,) + high.shape[1:], high.dtype)

        @pl.when(has_low)
        def _():
            pl.semaphore_wait(barrier, me)
            pl.semaphore_signal(next_ready, inc=1, device_id={"panel": me - 1})

        @pl.when(chip < last)
        def _():
            lax.fori_loop(0, me, answer, 0)

        @pl.when(chip == last)
        def _():
            lax.fori_loop(0, me, answer_last, 0)

        dens_copy.wait()
        cmap_copy.wait()
        for b in range(blk_count):
            own = cmap[b] - me * coarse_dev
            values = low[reach + b].astype(jnp.float32)
            rows = [values * (own == c).astype(jnp.float32) for c in range(coarse_dev)]
            masked[b] = jnp.concatenate(rows, axis=0).astype(jnp.bfloat16)

        def halo(up):
            return pltpu.make_async_remote_copy(
                src_ref=low.at[pl.ds(blk_count if up else reach, reach)],
                dst_ref=low.at[pl.ds(0, reach)] if up else high.at[pl.ds(blk_count, reach)],
                send_sem=halo_send.at[int(up)], recv_sem=halo_recv.at[int(up)],
                device_id={"panel": me + 1 if up else me - 1})

        @pl.when(has_low & (chip < last - 1))
        def _():
            halo(False).start()

        total = jnp.zeros((coarse_dev * columns, rest.shape[1]), jnp.float32)
        for i in range(PARTS):
            rest_copy(i).wait()
            blocks = range(i * part, (i + 1) * part)
            values = jnp.concatenate([masked[b] for b in blocks], axis=1)
            weights = jnp.concatenate([rest[b] for b in blocks], axis=1)
            total += lax.dot_general(values, weights, CONTRACT_LAST, preferred_element_type=jnp.float32)
        moments[me] = total.reshape(moments.shape[1:]).astype(jnp.bfloat16)

        def moment_copy(target, recv_sem):
            return pltpu.make_async_remote_copy(
                src_ref=moments.at[me], dst_ref=moments.at[me], send_sem=send_sem, recv_sem=recv_sem,
                device_id={"panel": target})

        def send(t, carry):
            moment_copy(t, early_recv).start()
            return carry

        def send_late(t, carry):
            moment_copy(t, late_recv).start()
            return carry

        @pl.when(chip < last)
        def _():
            lax.fori_loop(0, me, send, 0)

        @pl.when(chip == last)
        def _():
            lax.fori_loop(0, me, send_late, 0)

        @pl.when(chip >= last - 1)
        def _():
            halo(False).start()

        for k in range(PARTS):
            near_copy(lax.rem(k + (1 - core) * (PARTS // 2), PARTS)).start()
        eval_copy.start()

        @pl.when(has_high)
        def _():
            pl.semaphore_wait(next_ready, 1)
            halo(True).start()

        @pl.when(me < count - 3)
        def _():
            pl.semaphore_wait(ready, count - 3 - me)
            lax.fori_loop(me + 1, count - 2, send, 0)

        @pl.when(chip < last)
        def _():
            pl.semaphore_wait(last_ready, 2)
            lax.fori_loop(count - 2, count, send, 0)

        @pl.when(me == count - 2)
        def _():
            pl.semaphore_wait(last_ready, 1)
            send_late(count - 1, 0)

        neigh_copy.wait()
        live_copy.wait()
        high_copy.wait()
        half = PARTS // 2

        def near_half(field, first, base):
            def near_part(i, carry):
                near_copy(first + i).wait()
                for t in range(part):
                    b = (first + i) * part + t
                    alive = live[b]
                    places = [jnp.clip(neigh[j, b] - base, 0, zero_slot - 1) for j in range(slots)]
                    picked = [field[jnp.where(j < alive, places[j], zero_slot)] for j in range(slots)]
                    weights = jnp.concatenate([near[b, j] for j in range(slots)], axis=1)
                    acc[b] = lax.dot_general(jnp.concatenate(picked, axis=1), weights, CONTRACT_LAST,
                                             preferred_element_type=jnp.float32)
                return carry

            lax.fori_loop(0, half, near_part, 0)

        def low_half():
            @pl.when(has_low)
            def _():
                halo(True).wait_recv()

            near_half(low, 0, me * blk_count - reach)

        def high_half():
            @pl.when(has_high)
            def _():
                halo(False).wait_recv()

            near_half(high, half, me * blk_count)

        @pl.when(core == 1)
        def _():
            low_half()
            high_half()

        @pl.when(core == 0)
        def _():
            high_half()
            low_half()

        coup_copy.wait()
        eval_copy.wait()

        @pl.when(has_high)
        def _():
            halo(True).wait_send()

        @pl.when(has_low)
        def _():
            halo(False).wait_send()

        bytes_of(count - 1, send_sem).wait()

    dma = pltpu.SemaphoreType.DMA
    pl.run_scoped(gather, dma((7,)), dma((PARTS,)), dma((PARTS,)), dma((2,)), dma)

    @pl.when(chip < last)
    def _():
        bytes_of(count - 3, early_recv).wait()

    @pl.when(chip == last)
    def _():
        bytes_of(count - 2, early_recv).wait()

    sums = [jnp.zeros(moments.shape[2:], jnp.float32) for _ in range(coarse_dev)]

    def add(s):
        for i in range(coarse_dev):
            term = moments[s, i].astype(jnp.float32)
            for c in range(coarse_dev):
                sums[c] += coup[c, s * coarse_dev + i] * term

    for s in range(count - 2):
        add(s)

    @pl.when(chip < last)
    def _():
        bytes_of(2, late_recv).wait()

    @pl.when(chip == last)
    def _():
        bytes_of(1, late_recv).wait()

    add(count - 2)
    add(count - 1)
    spread = [total.astype(jnp.bfloat16) for total in sums]
    blank = jnp.zeros_like(spread[0])
    lhs = jnp.concatenate([jnp.concatenate([e, blank], axis=1) for e in spread]
                          + [jnp.concatenate([blank, e], axis=1) for e in spread], axis=0)
    for b0 in range(0, blk_count, 4):
        rhs = jnp.concatenate([jnp.concatenate([evl[b0 + i], evl[b0 + i + 1]], axis=1) for i in (0, 2)], axis=0)
        far = jnp.dot(lhs, rhs, preferred_element_type=jnp.float32)
        for i in range(4):
            b = b0 + i
            own = cmap[b] - me * coarse_dev
            lanes = slice((i % 2) * panels, (i % 2 + 1) * panels)
            first = (i // 2) * coarse_dev * columns
            part_far = far[first:first + columns, lanes]
            for c in range(1, coarse_dev):
                rows = first + c * columns
                part_far = jnp.where(own == c, far[rows:rows + columns, lanes], part_far)
            out[b] = (acc[b] + part_far).astype(jnp.bfloat16)


def shards(count, density, near_blocks, neighbours, counts, coarse_map, restrict, evaluate, coupling):
    blk_count, columns, panels = density.shape
    terms = restrict.shape[1]
    coarse_dev = coupling.shape[0]
    hbm = pl.BlockSpec(memory_space=pl.ANY)
    dma = pltpu.SemaphoreType.DMA
    return pl.pallas_call(
        functools.partial(kernel, count),
        out_shape=pltpu.VMEM(density.shape, jnp.bfloat16),
        in_specs=[hbm] * 8,
        out_specs=pl.BlockSpec(memory_space=pltpu.VMEM),
        scratch_shapes=[
            pltpu.SMEM(neighbours.shape[::-1], jnp.int32),
            pltpu.SMEM(counts.shape, jnp.int32),
            pltpu.SMEM(coarse_map.shape, jnp.int32),
            pltpu.SMEM(coupling.shape, jnp.float32),
            pltpu.VMEM((blk_count + blk_count // 2 + 1, columns, panels), jnp.bfloat16),
            pltpu.VMEM((blk_count + blk_count // 2 + 1, columns, panels), jnp.bfloat16),
            pltpu.VMEM(near_blocks.shape, jnp.bfloat16),
            pltpu.VMEM(restrict.shape, jnp.bfloat16),
            pltpu.VMEM(evaluate.shape, jnp.bfloat16),
            pltpu.VMEM((blk_count, coarse_dev * columns, panels), jnp.bfloat16),
            pltpu.VMEM((count, coarse_dev, columns, terms), jnp.bfloat16),
            pltpu.VMEM(density.shape, jnp.float32),
            dma((2,)),
            dma,
            dma,
            pltpu.SemaphoreType.REGULAR,
            pltpu.SemaphoreType.REGULAR,
            pltpu.SemaphoreType.REGULAR,
        ],
        compiler_params=pltpu.CompilerParams(collective_id=0, has_side_effects=True),
    )(density, near_blocks, neighbours.T, counts, coarse_map, restrict, evaluate, coupling)


def solution(mesh):
    rows = ("grp", "panel")
    placed = (
        P(rows, None, None),
        P(rows, None, None, None),
        P(rows, None),
        P(rows),
        P(rows),
        P(rows, None, None),
        P(rows, None, None),
        P(rows, None),
    )
    return jax.shard_map(
        functools.partial(shards, mesh.shape["panel"]),
        mesh=mesh,
        in_specs=placed,
        out_specs=P(rows, None, None),
        check_vma=False,
    )
```

```python
import functools

import jax
import jax.numpy as jnp
from jax import lax
from jax.experimental import pallas as pl
from jax.experimental.pallas import tpu as pltpu
from jax.sharding import PartitionSpec as P

PARTS = 4
REST_PARTS = 2
CONTRACT_LAST = (((1,), (1,)), ((), ()))


def kernel(count, dens_hbm, near_hbm, neigh_hbm, live_hbm, cmap_hbm, rest_hbm, eval_hbm, coup_hbm, out, neigh, live,
           cmap, coup, low, high, near, rest, evl, masked, moments, acc, halo_recv, early_recv, late_recv, next_ready, ready, last_ready):
    slots, blk_count = neigh.shape
    reach = blk_count // 2
    columns, panels = low.shape[1:]
    coarse_dev = moments.shape[1]
    zero_slot = low.shape[0] - 1
    chips = count // 2
    last = chips - 1
    part = blk_count // PARTS
    rest_part = blk_count // REST_PARTS
    me = lax.axis_index("panel")
    core = lax.rem(me, 2)
    chip = me // 2
    has_low = me > 0
    has_high = me < count - 1

    def bytes_of(n, sem):
        block = moments.at[pl.ds(0, n)]
        return pltpu.make_async_copy(block, block, sem)

    def gather(in_sem, rest_sem, near_sem, halo_send, send_sem):
        dens_copy = pltpu.make_async_copy(dens_hbm, low.at[pl.ds(reach, blk_count)], in_sem.at[0])
        high_copy = pltpu.make_async_copy(dens_hbm, high.at[pl.ds(0, blk_count)], in_sem.at[6])
        cmap_copy = pltpu.make_async_copy(cmap_hbm, cmap, in_sem.at[1])
        neigh_copy = pltpu.make_async_copy(neigh_hbm, neigh, in_sem.at[2])
        live_copy = pltpu.make_async_copy(live_hbm, live, in_sem.at[3])
        coup_copy = pltpu.make_async_copy(coup_hbm, coup, in_sem.at[4])
        eval_copy = pltpu.make_async_copy(eval_hbm, evl, in_sem.at[5])

        def rest_copy(i):
            blocks = pl.ds(i * rest_part, rest_part)
            return pltpu.make_async_copy(rest_hbm.at[blocks], rest.at[blocks], rest_sem.at[i])

        def near_copy(i):
            blocks = pl.ds(i * part, part)
            return pltpu.make_async_copy(near_hbm.at[blocks], near.at[blocks], near_sem.at[i])

        dens_copy.start()
        cmap_copy.start()
        for i in range(REST_PARTS):
            rest_copy(i).start()

        barrier = pltpu.get_barrier_semaphore()

        def greet(t, carry):
            pl.semaphore_signal(barrier, inc=1, device_id={"panel": t})
            return carry

        def answer(t, carry):
            pl.semaphore_signal(ready, inc=1, device_id={"panel": t})
            return carry

        def answer_last(t, carry):
            pl.semaphore_signal(last_ready, inc=1, device_id={"panel": t})
            return carry

        lax.fori_loop(me + 1, count, greet, 0)
        low[zero_slot] = jnp.zeros(low.shape[1:], low.dtype)
        high[zero_slot] = jnp.zeros(high.shape[1:], high.dtype)

        @pl.when(me == 0)
        def _():
            low[pl.ds(0, reach)] = jnp.zeros((reach,) + low.shape[1:], low.dtype)

        @pl.when(me == count - 1)
        def _():
            high[pl.ds(blk_count, reach)] = jnp.zeros((reach,) + high.shape[1:], high.dtype)

        def meet():
            pl.semaphore_wait(barrier, me)

        def reply(signal):
            pl.semaphore_signal(next_ready, inc=1, device_id={"panel": me - 1})
            lax.fori_loop(0, me, signal, 0)

        @pl.when(has_low & (chip < last))
        def _():
            meet()
            reply(answer)

        dens_copy.wait()
        cmap_copy.wait()
        for b in range(blk_count):
            own = cmap[b] - me * coarse_dev
            values = low[reach + b]
            masked[b] = jnp.concatenate(
                [jnp.where(own == c, values, jnp.zeros_like(values)) for c in range(coarse_dev)], axis=0)

        def halo(up):
            return pltpu.make_async_remote_copy(
                src_ref=low.at[pl.ds(blk_count if up else reach, reach)],
                dst_ref=low.at[pl.ds(0, reach)] if up else high.at[pl.ds(blk_count, reach)],
                send_sem=halo_send.at[int(up)], recv_sem=halo_recv.at[int(up)],
                device_id={"panel": me + 1 if up else me - 1})

        @pl.when(has_low & (chip < last - 1))
        def _():
            halo(False).start()

        total = jnp.zeros((coarse_dev * columns, rest.shape[1]), jnp.float32)
        for i in range(REST_PARTS):
            rest_copy(i).wait()
            blocks = range(i * rest_part, (i + 1) * rest_part)
            values = jnp.concatenate([masked[b] for b in blocks], axis=1)
            weights = jnp.concatenate([rest[b] for b in blocks], axis=1)
            total += lax.dot_general(values, weights, CONTRACT_LAST, preferred_element_type=jnp.float32)
        moments[me] = total.reshape(moments.shape[1:]).astype(jnp.bfloat16)

        high_copy.start()
        neigh_copy.start()
        live_copy.start()
        coup_copy.start()

        def moment_copy(target, recv_sem):
            return pltpu.make_async_remote_copy(
                src_ref=moments.at[me], dst_ref=moments.at[me], send_sem=send_sem, recv_sem=recv_sem,
                device_id={"panel": target})

        def send(t, carry):
            moment_copy(t, early_recv).start()
            return carry

        def send_late(t, carry):
            moment_copy(t, late_recv).start()
            return carry

        def send_down(first, stop):
            @pl.when(chip < last)
            def _():
                lax.fori_loop(first, stop, send, 0)

            @pl.when(chip == last)
            def _():
                lax.fori_loop(first, stop, send_late, 0)

        @pl.when(chip == last)
        def _():
            meet()

        send_down(0, jnp.minimum(me, 2))

        @pl.when(chip == last)
        def _():
            reply(answer_last)


        @pl.when(chip >= last - 1)
        def _():
            halo(False).start()

        for k in range(PARTS):
            near_copy(lax.rem(k + (1 - core) * (PARTS // 2), PARTS)).start()
        eval_copy.start()

        @pl.when(has_high)
        def _():
            pl.semaphore_wait(next_ready, 1)
            halo(True).start()

        send_down(2, me)

        def send_up():
            @pl.when(me < count - 3)
            def _():
                pl.semaphore_wait(ready, count - 3 - me)
                lax.fori_loop(me + 1, count - 2, send, 0)

            @pl.when(chip < last)
            def _():
                pl.semaphore_wait(last_ready, 2)
                lax.fori_loop(count - 2, count, send, 0)

            @pl.when(me == count - 2)
            def _():
                pl.semaphore_wait(last_ready, 1)
                send_late(count - 1, 0)

        @pl.when(chip > 0)
        def _():
            send_up()

        neigh_copy.wait()
        live_copy.wait()
        high_copy.wait()
        half = PARTS // 2

        def near_half(field, first, base):
            def near_part(i, carry):
                near_copy(first + i).wait()
                for t in range(part):
                    b = (first + i) * part + t
                    alive = live[b]
                    places = [jnp.clip(neigh[j, b] - base, 0, zero_slot - 1) for j in range(slots)]
                    picked = [field[jnp.where(j < alive, places[j], zero_slot)] for j in range(slots)]
                    weights = jnp.concatenate([near[b, j] for j in range(slots)], axis=1)
                    acc[b] = lax.dot_general(jnp.concatenate(picked, axis=1), weights, CONTRACT_LAST,
                                             preferred_element_type=jnp.float32)
                return carry

            lax.fori_loop(0, half, near_part, 0)

        def low_half():
            @pl.when(has_low)
            def _():
                halo(True).wait_recv()

            near_half(low, 0, me * blk_count - reach)

        def high_half():
            @pl.when(has_high)
            def _():
                halo(False).wait_recv()

            near_half(high, half, me * blk_count)

        @pl.when(core == 1)
        def _():
            low_half()

        @pl.when(core == 0)
        def _():
            high_half()

        @pl.when(chip == 0)
        def _():
            send_up()

        @pl.when(core == 1)
        def _():
            high_half()

        @pl.when(core == 0)
        def _():
            low_half()

        coup_copy.wait()
        eval_copy.wait()

        @pl.when(has_high)
        def _():
            halo(True).wait_send()

        @pl.when(has_low)
        def _():
            halo(False).wait_send()

        bytes_of(count - 1, send_sem).wait()

    dma = pltpu.SemaphoreType.DMA
    pl.run_scoped(gather, dma((7,)), dma((REST_PARTS,)), dma((PARTS,)), dma((2,)), dma)

    @pl.when(chip < last)
    def _():
        bytes_of(count - 3, early_recv).wait()

    @pl.when(chip == last)
    def _():
        bytes_of(count - 2, early_recv).wait()

    sums = [jnp.zeros(moments.shape[2:], jnp.float32) for _ in range(coarse_dev)]

    def add(s):
        for i in range(coarse_dev):
            term = moments[s, i].astype(jnp.float32)
            for c in range(coarse_dev):
                sums[c] += coup[c, s * coarse_dev + i] * term

    for s in range(count - 2):
        add(s)

    @pl.when(chip < last)
    def _():
        bytes_of(2, late_recv).wait()

    @pl.when(chip == last)
    def _():
        bytes_of(1, late_recv).wait()

    add(count - 2)
    add(count - 1)
    spread = [total.astype(jnp.bfloat16) for total in sums]
    blank = jnp.zeros_like(spread[0])
    lhs = jnp.concatenate([jnp.concatenate([e, blank], axis=1) for e in spread]
                          + [jnp.concatenate([blank, e], axis=1) for e in spread], axis=0)
    for b0 in range(0, blk_count, 4):
        rhs = jnp.concatenate([jnp.concatenate([evl[b0 + i], evl[b0 + i + 1]], axis=1) for i in (0, 2)], axis=0)
        far = jnp.dot(lhs, rhs, preferred_element_type=jnp.float32)
        for i in range(4):
            b = b0 + i
            own = cmap[b] - me * coarse_dev
            lanes = slice((i % 2) * panels, (i % 2 + 1) * panels)
            first = (i // 2) * coarse_dev * columns
            part_far = far[first:first + columns, lanes]
            for c in range(1, coarse_dev):
                rows = first + c * columns
                part_far = jnp.where(own == c, far[rows:rows + columns, lanes], part_far)
            out[b] = (acc[b] + part_far).astype(jnp.bfloat16)


def shards(count, density, near_blocks, neighbours, counts, coarse_map, restrict, evaluate, coupling):
    blk_count, columns, panels = density.shape
    terms = restrict.shape[1]
    coarse_dev = coupling.shape[0]
    hbm = pl.BlockSpec(memory_space=pl.ANY)
    dma = pltpu.SemaphoreType.DMA
    return pl.pallas_call(
        functools.partial(kernel, count),
        out_shape=pltpu.VMEM(density.shape, jnp.bfloat16),
        in_specs=[hbm] * 8,
        out_specs=pl.BlockSpec(memory_space=pltpu.VMEM),
        scratch_shapes=[
            pltpu.SMEM(neighbours.shape[::-1], jnp.int32),
            pltpu.SMEM(counts.shape, jnp.int32),
            pltpu.SMEM(coarse_map.shape, jnp.int32),
            pltpu.SMEM(coupling.shape, jnp.float32),
            pltpu.VMEM((blk_count + blk_count // 2 + 1, columns, panels), jnp.bfloat16),
            pltpu.VMEM((blk_count + blk_count // 2 + 1, columns, panels), jnp.bfloat16),
            pltpu.VMEM(near_blocks.shape, jnp.bfloat16),
            pltpu.VMEM(restrict.shape, jnp.bfloat16),
            pltpu.VMEM(evaluate.shape, jnp.bfloat16),
            pltpu.VMEM((blk_count, coarse_dev * columns, panels), jnp.bfloat16),
            pltpu.VMEM((count, coarse_dev, columns, terms), jnp.bfloat16),
            pltpu.VMEM(density.shape, jnp.float32),
            dma((2,)),
            dma,
            dma,
            pltpu.SemaphoreType.REGULAR,
            pltpu.SemaphoreType.REGULAR,
            pltpu.SemaphoreType.REGULAR,
        ],
        compiler_params=pltpu.CompilerParams(collective_id=0, has_side_effects=True),
    )(density, near_blocks, neighbours.T, counts, coarse_map, restrict, evaluate, coupling)


def solution(mesh):
    rows = ("grp", "panel")
    placed = (
        P(rows, None, None),
        P(rows, None, None, None),
        P(rows, None),
        P(rows),
        P(rows),
        P(rows, None, None),
        P(rows, None, None),
        P(rows, None),
    )
    return jax.shard_map(
        functools.partial(shards, mesh.shape["panel"]),
        mesh=mesh,
        in_specs=placed,
        out_specs=P(rows, None, None),
        check_vma=False,
    )
```

```python
import functools

import jax
import jax.numpy as jnp
from jax import lax
from jax.experimental import pallas as pl
from jax.experimental.pallas import tpu as pltpu
from jax.sharding import PartitionSpec as P

PARTS = 4
REST_PARTS = 2
CONTRACT_LAST = (((1,), (1,)), ((), ()))


def kernel(count, dens_hbm, near_hbm, neigh_hbm, live_hbm, cmap_hbm, rest_hbm, eval_hbm, coup_hbm, out, neigh, live,
           cmap, coup, low, high, near, rest, evl, masked, moments, acc, late_recv):
    slots, blk_count = neigh.shape
    reach = blk_count // 2
    columns, panels = low.shape[1:]
    coarse_dev = moments.shape[1]
    zero_slot = low.shape[0] - 1
    chips = count // 2
    last = chips - 1
    part = blk_count // PARTS
    rest_part = blk_count // REST_PARTS
    me = lax.axis_index("panel")
    core = lax.rem(me, 2)
    chip = me // 2
    has_low = me > 0
    has_high = me < count - 1

    def bytes_of(n, sem):
        block = moments.at[pl.ds(0, n)]
        return pltpu.make_async_copy(block, block, sem)

    def gather(in_sem, rest_sem, near_sem, halo_send, send_sem, halo_recv, early_recv, next_ready, ready, last_ready):
        dens_copy = pltpu.make_async_copy(dens_hbm, low.at[pl.ds(reach, blk_count)], in_sem.at[0])
        high_copy = pltpu.make_async_copy(dens_hbm, high.at[pl.ds(0, blk_count)], in_sem.at[6])
        cmap_copy = pltpu.make_async_copy(cmap_hbm, cmap, in_sem.at[1])
        neigh_copy = pltpu.make_async_copy(neigh_hbm, neigh, in_sem.at[2])
        live_copy = pltpu.make_async_copy(live_hbm, live, in_sem.at[3])
        coup_copy = pltpu.make_async_copy(coup_hbm, coup, in_sem.at[4])
        eval_copy = pltpu.make_async_copy(eval_hbm, evl, in_sem.at[5])

        def rest_copy(i):
            blocks = pl.ds(i * rest_part, rest_part)
            return pltpu.make_async_copy(rest_hbm.at[blocks], rest.at[blocks], rest_sem.at[i])

        def near_copy(i):
            blocks = pl.ds(i * part, part)
            return pltpu.make_async_copy(near_hbm.at[blocks], near.at[blocks], near_sem.at[i])

        dens_copy.start()
        cmap_copy.start()
        for i in range(REST_PARTS):
            rest_copy(i).start()

        barrier = pltpu.get_barrier_semaphore()

        def greet(t, carry):
            pl.semaphore_signal(barrier, inc=1, device_id={"panel": t})
            return carry

        def answer(t, carry):
            pl.semaphore_signal(ready, inc=1, device_id={"panel": t})
            return carry

        def answer_last(t, carry):
            pl.semaphore_signal(last_ready, inc=1, device_id={"panel": t})
            return carry

        lax.fori_loop(me + 1, count, greet, 0)
        low[zero_slot] = jnp.zeros(low.shape[1:], low.dtype)
        high[zero_slot] = jnp.zeros(high.shape[1:], high.dtype)

        @pl.when(me == 0)
        def _():
            low[pl.ds(0, reach)] = jnp.zeros((reach,) + low.shape[1:], low.dtype)

        @pl.when(me == count - 1)
        def _():
            high[pl.ds(blk_count, reach)] = jnp.zeros((reach,) + high.shape[1:], high.dtype)

        def meet():
            pl.semaphore_wait(barrier, me)

        def reply(signal):
            pl.semaphore_signal(next_ready, inc=1, device_id={"panel": me - 1})
            lax.fori_loop(0, me, signal, 0)

        @pl.when(has_low & (chip < last))
        def _():
            meet()
            reply(answer)

        dens_copy.wait()
        cmap_copy.wait()
        for b in range(blk_count):
            own = cmap[b] - me * coarse_dev
            values = low[reach + b]
            masked[b] = jnp.concatenate(
                [jnp.where(own == c, values, jnp.zeros_like(values)) for c in range(coarse_dev)], axis=0)

        def halo(up):
            return pltpu.make_async_remote_copy(
                src_ref=low.at[pl.ds(blk_count if up else reach, reach)],
                dst_ref=low.at[pl.ds(0, reach)] if up else high.at[pl.ds(blk_count, reach)],
                send_sem=halo_send.at[int(up)], recv_sem=halo_recv.at[int(up)],
                device_id={"panel": me + 1 if up else me - 1})

        @pl.when(has_low & (chip < last - 1))
        def _():
            halo(False).start()

        total = jnp.zeros((coarse_dev * columns, rest.shape[1]), jnp.float32)
        for i in range(REST_PARTS):
            rest_copy(i).wait()
            blocks = range(i * rest_part, (i + 1) * rest_part)
            values = jnp.concatenate([masked[b] for b in blocks], axis=1)
            weights = jnp.concatenate([rest[b] for b in blocks], axis=1)
            total += lax.dot_general(values, weights, CONTRACT_LAST, preferred_element_type=jnp.float32)
        moments[me] = total.reshape(moments.shape[1:]).astype(jnp.bfloat16)

        high_copy.start()
        neigh_copy.start()
        live_copy.start()
        coup_copy.start()

        def moment_copy(target, recv_sem):
            return pltpu.make_async_remote_copy(
                src_ref=moments.at[me], dst_ref=moments.at[me], send_sem=send_sem, recv_sem=recv_sem,
                device_id={"panel": target})

        def send(t, carry):
            moment_copy(t, early_recv).start()
            return carry

        def send_late(t, carry):
            moment_copy(t, late_recv).start()
            return carry

        def send_down(first, stop):
            @pl.when(chip < last)
            def _():
                lax.fori_loop(first, stop, send, 0)

            @pl.when(chip == last)
            def _():
                lax.fori_loop(first, stop, send_late, 0)

        @pl.when(chip == last)
        def _():
            meet()

        send_down(0, jnp.minimum(me, 2))

        @pl.when(chip == last)
        def _():
            reply(answer_last)


        @pl.when(chip >= last - 1)
        def _():
            halo(False).start()

        for k in range(PARTS):
            near_copy(lax.rem(k + (1 - core) * (PARTS // 2), PARTS)).start()
        eval_copy.start()

        @pl.when(has_high)
        def _():
            pl.semaphore_wait(next_ready, 1)
            halo(True).start()

        send_down(2, me)

        def send_up():
            @pl.when(me < count - 3)
            def _():
                pl.semaphore_wait(ready, count - 3 - me)
                lax.fori_loop(me + 1, count - 2, send, 0)

            @pl.when(chip < last)
            def _():
                pl.semaphore_wait(last_ready, 2)
                lax.fori_loop(count - 2, count, send, 0)

            @pl.when(me == count - 2)
            def _():
                pl.semaphore_wait(last_ready, 1)
                send_late(count - 1, 0)

        @pl.when(chip > 0)
        def _():
            send_up()

        neigh_copy.wait()
        live_copy.wait()
        high_copy.wait()
        half = PARTS // 2

        def near_half(field, first, base):
            def near_part(i, carry):
                near_copy(first + i).wait()
                for t in range(part):
                    b = (first + i) * part + t
                    alive = live[b]
                    places = [jnp.clip(neigh[j, b] - base, 0, zero_slot - 1) for j in range(slots)]
                    picked = [field[jnp.where(j < alive, places[j], zero_slot)] for j in range(slots)]
                    weights = jnp.concatenate([near[b, j] for j in range(slots)], axis=1)
                    acc[b] = lax.dot_general(jnp.concatenate(picked, axis=1), weights, CONTRACT_LAST,
                                             preferred_element_type=jnp.float32)
                return carry

            lax.fori_loop(0, half, near_part, 0)

        def low_half():
            @pl.when(has_low)
            def _():
                halo(True).wait_recv()

            near_half(low, 0, me * blk_count - reach)

        def high_half():
            @pl.when(has_high)
            def _():
                halo(False).wait_recv()

            near_half(high, half, me * blk_count)

        @pl.when(core == 1)
        def _():
            low_half()

        @pl.when(core == 0)
        def _():
            high_half()

        @pl.when(chip == 0)
        def _():
            send_up()

        @pl.when(core == 1)
        def _():
            high_half()

        @pl.when(core == 0)
        def _():
            low_half()

        coup_copy.wait()
        eval_copy.wait()

        @pl.when(has_high)
        def _():
            halo(True).wait_send()

        @pl.when(has_low)
        def _():
            halo(False).wait_send()

        bytes_of(count - 1, send_sem).wait()

        @pl.when(chip < last)
        def _():
            bytes_of(count - 3, early_recv).wait()

        @pl.when(chip == last)
        def _():
            bytes_of(count - 2, early_recv).wait()

    dma, signal = pltpu.SemaphoreType.DMA, pltpu.SemaphoreType.REGULAR
    pl.run_scoped(gather, dma((7,)), dma((REST_PARTS,)), dma((PARTS,)), dma((2,)), dma, dma((2,)), dma,
                  signal, signal, signal)

    sums = [jnp.zeros(moments.shape[2:], jnp.float32) for _ in range(coarse_dev)]

    def add(s):
        for i in range(coarse_dev):
            term = moments[s, i].astype(jnp.float32)
            for c in range(coarse_dev):
                sums[c] += coup[c, s * coarse_dev + i] * term

    for s in range(count - 2):
        add(s)

    @pl.when(chip < last)
    def _():
        bytes_of(2, late_recv).wait()

    @pl.when(chip == last)
    def _():
        bytes_of(1, late_recv).wait()

    add(count - 2)
    add(count - 1)
    spread = [total.astype(jnp.bfloat16) for total in sums]
    blank = jnp.zeros_like(spread[0])
    lhs = jnp.concatenate([jnp.concatenate([e, blank], axis=1) for e in spread]
                          + [jnp.concatenate([blank, e], axis=1) for e in spread], axis=0)
    for b0 in range(0, blk_count, 4):
        rhs = jnp.concatenate([jnp.concatenate([evl[b0 + i], evl[b0 + i + 1]], axis=1) for i in (0, 2)], axis=0)
        far = jnp.dot(lhs, rhs, preferred_element_type=jnp.float32)
        for i in range(4):
            b = b0 + i
            own = cmap[b] - me * coarse_dev
            lanes = slice((i % 2) * panels, (i % 2 + 1) * panels)
            first = (i // 2) * coarse_dev * columns
            part_far = far[first:first + columns, lanes]
            for c in range(1, coarse_dev):
                rows = first + c * columns
                part_far = jnp.where(own == c, far[rows:rows + columns, lanes], part_far)
            out[b] = (acc[b] + part_far).astype(jnp.bfloat16)


def shards(count, density, near_blocks, neighbours, counts, coarse_map, restrict, evaluate, coupling):
    blk_count, columns, panels = density.shape
    terms = restrict.shape[1]
    coarse_dev = coupling.shape[0]
    hbm = pl.BlockSpec(memory_space=pl.ANY)
    dma = pltpu.SemaphoreType.DMA
    return pl.pallas_call(
        functools.partial(kernel, count),
        out_shape=pltpu.VMEM(density.shape, jnp.bfloat16),
        in_specs=[hbm] * 8,
        out_specs=pl.BlockSpec(memory_space=pltpu.VMEM),
        scratch_shapes=[
            pltpu.SMEM(neighbours.shape[::-1], jnp.int32),
            pltpu.SMEM(counts.shape, jnp.int32),
            pltpu.SMEM(coarse_map.shape, jnp.int32),
            pltpu.SMEM(coupling.shape, jnp.float32),
            pltpu.VMEM((blk_count + blk_count // 2 + 1, columns, panels), jnp.bfloat16),
            pltpu.VMEM((blk_count + blk_count // 2 + 1, columns, panels), jnp.bfloat16),
            pltpu.VMEM(near_blocks.shape, jnp.bfloat16),
            pltpu.VMEM(restrict.shape, jnp.bfloat16),
            pltpu.VMEM(evaluate.shape, jnp.bfloat16),
            pltpu.VMEM((blk_count, coarse_dev * columns, panels), jnp.bfloat16),
            pltpu.VMEM((count, coarse_dev, columns, terms), jnp.bfloat16),
            pltpu.VMEM(density.shape, jnp.float32),
            dma,
        ],
        compiler_params=pltpu.CompilerParams(collective_id=0, has_side_effects=True),
    )(density, near_blocks, neighbours.T, counts, coarse_map, restrict, evaluate, coupling)


def solution(mesh):
    rows = ("grp", "panel")
    placed = (
        P(rows, None, None),
        P(rows, None, None, None),
        P(rows, None),
        P(rows),
        P(rows),
        P(rows, None, None),
        P(rows, None, None),
        P(rows, None),
    )
    return jax.shard_map(
        functools.partial(shards, mesh.shape["panel"]),
        mesh=mesh,
        in_specs=placed,
        out_specs=P(rows, None, None),
        check_vma=False,
    )
```

```python
import functools

import jax
import jax.numpy as jnp
from jax import lax
from jax.experimental import pallas as pl
from jax.experimental.pallas import tpu as pltpu
from jax.sharding import PartitionSpec as P

PARTS = 4
REST_CUTS = (0, 12, 32)
CONTRACT_LAST = (((1,), (1,)), ((), ()))


def kernel(count, dens_hbm, near_hbm, neigh_hbm, live_hbm, cmap_hbm, rest_hbm, eval_hbm, coup_hbm, out, neigh, live,
           cmap, coup, low, high, near, rest, evl, masked, partial, moments, acc, late_recv):
    slots, blk_count = neigh.shape
    reach = blk_count // 2
    columns, panels = low.shape[1:]
    coarse_dev = moments.shape[1]
    zero_slot = low.shape[0] - 1
    chips = count // 2
    last = chips - 1
    part = blk_count // PARTS
    cuts = [blk_count * cut // 32 for cut in REST_CUTS]
    rest_parts = len(cuts) - 1
    me = lax.axis_index("panel")
    core = lax.rem(me, 2)
    chip = me // 2
    has_low = me > 0
    has_high = me < count - 1

    def bytes_of(n, sem):
        block = moments.at[pl.ds(0, n)]
        return pltpu.make_async_copy(block, block, sem)

    def gather(in_sem, rest_sem, near_sem, halo_send, send_sem, halo_recv, early_recv, next_ready, ready, last_ready):
        dens_copy = pltpu.make_async_copy(dens_hbm, low.at[pl.ds(reach, blk_count)], in_sem.at[0])
        high_copy = pltpu.make_async_copy(dens_hbm, high.at[pl.ds(0, blk_count)], in_sem.at[6])
        cmap_copy = pltpu.make_async_copy(cmap_hbm, cmap, in_sem.at[1])
        neigh_copy = pltpu.make_async_copy(neigh_hbm, neigh, in_sem.at[2])
        live_copy = pltpu.make_async_copy(live_hbm, live, in_sem.at[3])
        coup_copy = pltpu.make_async_copy(coup_hbm, coup, in_sem.at[4])
        eval_copy = pltpu.make_async_copy(eval_hbm, evl, in_sem.at[5])

        def rest_copy(i):
            blocks = pl.ds(cuts[i], cuts[i + 1] - cuts[i])
            return pltpu.make_async_copy(rest_hbm.at[blocks], rest.at[blocks], rest_sem.at[i])

        def near_copy(i):
            blocks = pl.ds(i * part, part)
            return pltpu.make_async_copy(near_hbm.at[blocks], near.at[blocks], near_sem.at[i])

        dens_copy.start()
        cmap_copy.start()
        for i in range(rest_parts):
            rest_copy(i).start()

        barrier = pltpu.get_barrier_semaphore()

        def greet(t, carry):
            pl.semaphore_signal(barrier, inc=1, device_id={"panel": t})
            return carry

        def answer(t, carry):
            pl.semaphore_signal(ready, inc=1, device_id={"panel": t})
            return carry

        def answer_last(t, carry):
            pl.semaphore_signal(last_ready, inc=1, device_id={"panel": t})
            return carry

        lax.fori_loop(me + 1, count, greet, 0)
        low[zero_slot] = jnp.zeros(low.shape[1:], low.dtype)
        high[zero_slot] = jnp.zeros(high.shape[1:], high.dtype)

        @pl.when(me == 0)
        def _():
            low[pl.ds(0, reach)] = jnp.zeros((reach,) + low.shape[1:], low.dtype)

        @pl.when(me == count - 1)
        def _():
            high[pl.ds(blk_count, reach)] = jnp.zeros((reach,) + high.shape[1:], high.dtype)

        def meet():
            pl.semaphore_wait(barrier, me)

        def reply(signal):
            pl.semaphore_signal(next_ready, inc=1, device_id={"panel": me - 1})
            lax.fori_loop(0, me, signal, 0)

        @pl.when(has_low & (chip < last))
        def _():
            meet()
            reply(answer)

        dens_copy.wait()
        cmap_copy.wait()
        for b in range(blk_count):
            own = cmap[b] - me * coarse_dev
            values = low[reach + b]
            masked[b] = jnp.concatenate(
                [jnp.where(own == c, values, jnp.zeros_like(values)) for c in range(coarse_dev)], axis=0)

        def halo(up):
            return pltpu.make_async_remote_copy(
                src_ref=low.at[pl.ds(blk_count if up else reach, reach)],
                dst_ref=low.at[pl.ds(0, reach)] if up else high.at[pl.ds(blk_count, reach)],
                send_sem=halo_send.at[int(up)], recv_sem=halo_recv.at[int(up)],
                device_id={"panel": me + 1 if up else me - 1})

        @pl.when(has_low & (chip < last - 1))
        def _():
            halo(False).start()

        def terms_of(i):
            rest_copy(i).wait()
            blocks = range(cuts[i], cuts[i + 1])
            values = jnp.concatenate([masked[b] for b in blocks], axis=1)
            weights = jnp.concatenate([rest[b] for b in blocks], axis=1)
            return lax.dot_general(values, weights, CONTRACT_LAST, preferred_element_type=jnp.float32)

        partial[...] = jnp.zeros(partial.shape, partial.dtype)
        for i in range(rest_parts - 1):
            @pl.when(me >= 0)
            def _(i=i):
                partial[...] += terms_of(i)

        total = partial[...] + terms_of(rest_parts - 1)
        moments[me] = total.reshape(moments.shape[1:]).astype(jnp.bfloat16)

        high_copy.start()
        neigh_copy.start()
        live_copy.start()
        coup_copy.start()

        def moment_copy(target, recv_sem):
            return pltpu.make_async_remote_copy(
                src_ref=moments.at[me], dst_ref=moments.at[me], send_sem=send_sem, recv_sem=recv_sem,
                device_id={"panel": target})

        def send(t, carry):
            moment_copy(t, early_recv).start()
            return carry

        def send_late(t, carry):
            moment_copy(t, late_recv).start()
            return carry

        def send_down(first, stop):
            @pl.when(chip < last)
            def _():
                lax.fori_loop(first, stop, send, 0)

            @pl.when(chip == last)
            def _():
                lax.fori_loop(first, stop, send_late, 0)

        @pl.when(chip == last)
        def _():
            meet()
            send_late(0, 0)
            send_late(1, 0)
            reply(answer_last)

        @pl.when(chip < last)
        def _():
            lax.fori_loop(0, jnp.minimum(me, 2), send, 0)


        @pl.when(chip >= last - 1)
        def _():
            halo(False).start()

        for k in range(PARTS):
            near_copy(lax.rem(k + (1 - core) * (PARTS // 2), PARTS)).start()
        eval_copy.start()

        @pl.when(has_high)
        def _():
            pl.semaphore_wait(next_ready, 1)
            halo(True).start()

        send_down(2, me)

        def send_up():
            @pl.when(me < count - 3)
            def _():
                pl.semaphore_wait(ready, count - 3 - me)
                lax.fori_loop(me + 1, count - 2, send, 0)

            @pl.when(chip < last)
            def _():
                pl.semaphore_wait(last_ready, 2)
                lax.fori_loop(count - 2, count, send, 0)

            @pl.when(me == count - 2)
            def _():
                pl.semaphore_wait(last_ready, 1)
                send_late(count - 1, 0)

        @pl.when(chip > 0)
        def _():
            send_up()

        neigh_copy.wait()
        live_copy.wait()
        high_copy.wait()
        half = PARTS // 2

        def near_half(field, first, base):
            def near_part(i, carry):
                near_copy(first + i).wait()
                for t in range(part):
                    b = (first + i) * part + t
                    alive = live[b]
                    places = [jnp.clip(neigh[j, b] - base, 0, zero_slot - 1) for j in range(slots)]
                    picked = [field[jnp.where(j < alive, places[j], zero_slot)] for j in range(slots)]
                    weights = jnp.concatenate([near[b, j] for j in range(slots)], axis=1)
                    acc[b] = lax.dot_general(jnp.concatenate(picked, axis=1), weights, CONTRACT_LAST,
                                             preferred_element_type=jnp.float32)
                return carry

            lax.fori_loop(0, half, near_part, 0)

        def low_half():
            @pl.when(has_low)
            def _():
                halo(True).wait_recv()

            near_half(low, 0, me * blk_count - reach)

        def high_half():
            @pl.when(has_high)
            def _():
                halo(False).wait_recv()

            near_half(high, half, me * blk_count)

        @pl.when(core == 1)
        def _():
            low_half()

        @pl.when(core == 0)
        def _():
            high_half()

        @pl.when(chip == 0)
        def _():
            send_up()

        @pl.when(core == 1)
        def _():
            high_half()

        @pl.when(core == 0)
        def _():
            low_half()

        coup_copy.wait()
        eval_copy.wait()

        @pl.when(has_high)
        def _():
            halo(True).wait_send()

        @pl.when(has_low)
        def _():
            halo(False).wait_send()

        bytes_of(count - 1, send_sem).wait()

        @pl.when(chip < last)
        def _():
            bytes_of(count - 3, early_recv).wait()

        @pl.when(chip == last)
        def _():
            bytes_of(count - 2, early_recv).wait()

    dma, signal = pltpu.SemaphoreType.DMA, pltpu.SemaphoreType.REGULAR
    pl.run_scoped(gather, dma((7,)), dma((rest_parts,)), dma((PARTS,)), dma((2,)), dma, dma((2,)), dma,
                  signal, signal, signal)

    sums = [jnp.zeros(moments.shape[2:], jnp.float32) for _ in range(coarse_dev)]

    def weights_of(s):
        return [[coup[c, s * coarse_dev + i] for c in range(coarse_dev)] for i in range(coarse_dev)]

    def add(s, factors):
        for i in range(coarse_dev):
            term = moments[s, i].astype(jnp.float32)
            for c in range(coarse_dev):
                sums[c] += factors[i][c] * term

    for s in range(count - 2):
        add(s, weights_of(s))
    late_factors = [weights_of(s) for s in (count - 2, count - 1)]

    @pl.when(chip < last)
    def _():
        bytes_of(2, late_recv).wait()

    @pl.when(chip == last)
    def _():
        bytes_of(1, late_recv).wait()

    add(count - 2, late_factors[0])
    add(count - 1, late_factors[1])
    spread = [total.astype(jnp.bfloat16) for total in sums]
    blank = jnp.zeros_like(spread[0])
    lhs = jnp.concatenate([jnp.concatenate([e, blank], axis=1) for e in spread]
                          + [jnp.concatenate([blank, e], axis=1) for e in spread], axis=0)
    for b0 in range(0, blk_count, 4):
        rhs = jnp.concatenate([jnp.concatenate([evl[b0 + i], evl[b0 + i + 1]], axis=1) for i in (0, 2)], axis=0)
        far = jnp.dot(lhs, rhs, preferred_element_type=jnp.float32)
        for i in range(4):
            b = b0 + i
            own = cmap[b] - me * coarse_dev
            lanes = slice((i % 2) * panels, (i % 2 + 1) * panels)
            first = (i // 2) * coarse_dev * columns
            part_far = far[first:first + columns, lanes]
            for c in range(1, coarse_dev):
                rows = first + c * columns
                part_far = jnp.where(own == c, far[rows:rows + columns, lanes], part_far)
            out[b] = (acc[b] + part_far).astype(jnp.bfloat16)


def shards(count, density, near_blocks, neighbours, counts, coarse_map, restrict, evaluate, coupling):
    blk_count, columns, panels = density.shape
    terms = restrict.shape[1]
    coarse_dev = coupling.shape[0]
    hbm = pl.BlockSpec(memory_space=pl.ANY)
    dma = pltpu.SemaphoreType.DMA
    return pl.pallas_call(
        functools.partial(kernel, count),
        out_shape=pltpu.VMEM(density.shape, jnp.bfloat16),
        in_specs=[hbm] * 8,
        out_specs=pl.BlockSpec(memory_space=pltpu.VMEM),
        scratch_shapes=[
            pltpu.SMEM(neighbours.shape[::-1], jnp.int32),
            pltpu.SMEM(counts.shape, jnp.int32),
            pltpu.SMEM(coarse_map.shape, jnp.int32),
            pltpu.SMEM(coupling.shape, jnp.float32),
            pltpu.VMEM((blk_count + blk_count // 2 + 1, columns, panels), jnp.bfloat16),
            pltpu.VMEM((blk_count + blk_count // 2 + 1, columns, panels), jnp.bfloat16),
            pltpu.VMEM(near_blocks.shape, jnp.bfloat16),
            pltpu.VMEM(restrict.shape, jnp.bfloat16),
            pltpu.VMEM(evaluate.shape, jnp.bfloat16),
            pltpu.VMEM((blk_count, coarse_dev * columns, panels), jnp.bfloat16),
            pltpu.VMEM((coarse_dev * columns, terms), jnp.float32),
            pltpu.VMEM((count, coarse_dev, columns, terms), jnp.bfloat16),
            pltpu.VMEM(density.shape, jnp.float32),
            dma,
        ],
        compiler_params=pltpu.CompilerParams(collective_id=0, has_side_effects=True),
    )(density, near_blocks, neighbours.T, counts, coarse_map, restrict, evaluate, coupling)


def solution(mesh):
    rows = ("grp", "panel")
    placed = (
        P(rows, None, None),
        P(rows, None, None, None),
        P(rows, None),
        P(rows),
        P(rows),
        P(rows, None, None),
        P(rows, None, None),
        P(rows, None),
    )
    return jax.shard_map(
        functools.partial(shards, mesh.shape["panel"]),
        mesh=mesh,
        in_specs=placed,
        out_specs=P(rows, None, None),
        check_vma=False,
    )
```

```python
import functools

import jax
import jax.numpy as jnp
from jax import lax
from jax.experimental import pallas as pl
from jax.experimental.pallas import tpu as pltpu
from jax.sharding import PartitionSpec as P

PARTS = 4
REST_CUTS = (0, 12, 32)
CONTRACT_LAST = (((1,), (1,)), ((), ()))


def kernel(count, dens_hbm, near_hbm, neigh_hbm, live_hbm, cmap_hbm, rest_hbm, eval_hbm, coup_hbm, out, neigh, live,
           cmap, coup, low, high, near, rest, evl, masked, partial, moments, acc, late_recv):
    slots, blk_count = neigh.shape
    reach = blk_count // 2
    columns, panels = low.shape[1:]
    coarse_dev = moments.shape[1]
    zero_slot = low.shape[0] - 1
    chips = count // 2
    last = chips - 1
    part = blk_count // PARTS
    cuts = [blk_count * cut // 32 for cut in REST_CUTS]
    rest_parts = len(cuts) - 1
    me = lax.axis_index("panel")
    core = lax.rem(me, 2)
    chip = me // 2
    has_low = me > 0
    has_high = me < count - 1

    def bytes_of(n, sem):
        block = moments.at[pl.ds(0, n)]
        return pltpu.make_async_copy(block, block, sem)

    def gather(in_sem, rest_sem, near_sem, halo_send, send_sem, halo_recv, early_recv, next_ready, ready, last_ready):
        dens_copy = pltpu.make_async_copy(dens_hbm, low.at[pl.ds(reach, blk_count)], in_sem.at[0])
        high_copy = pltpu.make_async_copy(dens_hbm, high.at[pl.ds(0, blk_count)], in_sem.at[6])
        cmap_copy = pltpu.make_async_copy(cmap_hbm, cmap, in_sem.at[1])
        neigh_copy = pltpu.make_async_copy(neigh_hbm, neigh, in_sem.at[2])
        live_copy = pltpu.make_async_copy(live_hbm, live, in_sem.at[3])
        coup_copy = pltpu.make_async_copy(coup_hbm, coup, in_sem.at[4])
        eval_copy = pltpu.make_async_copy(eval_hbm, evl, in_sem.at[5])

        def rest_copy(i):
            blocks = pl.ds(cuts[i], cuts[i + 1] - cuts[i])
            return pltpu.make_async_copy(rest_hbm.at[blocks], rest.at[blocks], rest_sem.at[i])

        def near_copy(i):
            blocks = pl.ds(i * part, part)
            return pltpu.make_async_copy(near_hbm.at[blocks], near.at[blocks], near_sem.at[i])

        rest_copy(0).start()
        dens_copy.start()
        cmap_copy.start()
        for i in range(1, rest_parts):
            rest_copy(i).start()

        barrier = pltpu.get_barrier_semaphore()

        def greet(t, carry):
            pl.semaphore_signal(barrier, inc=1, device_id={"panel": t})
            return carry

        def answer(t, carry):
            pl.semaphore_signal(ready, inc=1, device_id={"panel": t})
            return carry

        def answer_last(t, carry):
            pl.semaphore_signal(last_ready, inc=1, device_id={"panel": t})
            return carry

        lax.fori_loop(me + 1, count, greet, 0)
        low[zero_slot] = jnp.zeros(low.shape[1:], low.dtype)
        high[zero_slot] = jnp.zeros(high.shape[1:], high.dtype)

        @pl.when(me == 0)
        def _():
            low[pl.ds(0, reach)] = jnp.zeros((reach,) + low.shape[1:], low.dtype)

        @pl.when(me == count - 1)
        def _():
            high[pl.ds(blk_count, reach)] = jnp.zeros((reach,) + high.shape[1:], high.dtype)

        def meet():
            pl.semaphore_wait(barrier, me)

        def reply(signal):
            pl.semaphore_signal(next_ready, inc=1, device_id={"panel": me - 1})
            lax.fori_loop(0, me, signal, 0)

        @pl.when(has_low & (chip < last))
        def _():
            meet()
            reply(answer)

        dens_copy.wait()
        cmap_copy.wait()
        for b in range(blk_count):
            own = cmap[b] - me * coarse_dev
            values = low[reach + b]
            masked[b] = jnp.concatenate(
                [jnp.where(own == c, values, jnp.zeros_like(values)) for c in range(coarse_dev)], axis=0)

        def halo(up):
            return pltpu.make_async_remote_copy(
                src_ref=low.at[pl.ds(blk_count if up else reach, reach)],
                dst_ref=low.at[pl.ds(0, reach)] if up else high.at[pl.ds(blk_count, reach)],
                send_sem=halo_send.at[int(up)], recv_sem=halo_recv.at[int(up)],
                device_id={"panel": me + 1 if up else me - 1})

        @pl.when(has_low & (chip < last - 1))
        def _():
            halo(False).start()

        def terms_of(i):
            rest_copy(i).wait()
            blocks = range(cuts[i], cuts[i + 1])
            values = jnp.concatenate([masked[b] for b in blocks], axis=1)
            weights = jnp.concatenate([rest[b] for b in blocks], axis=1)
            return lax.dot_general(values, weights, CONTRACT_LAST, preferred_element_type=jnp.float32)

        partial[...] = jnp.zeros(partial.shape, partial.dtype)
        for i in range(rest_parts - 1):
            @pl.when(me >= 0)
            def _(i=i):
                partial[...] += terms_of(i)

        total = partial[...] + terms_of(rest_parts - 1)
        moments[me] = total.reshape(moments.shape[1:]).astype(jnp.bfloat16)

        high_copy.start()
        neigh_copy.start()
        live_copy.start()
        coup_copy.start()

        def moment_copy(target, recv_sem):
            return pltpu.make_async_remote_copy(
                src_ref=moments.at[me], dst_ref=moments.at[me], send_sem=send_sem, recv_sem=recv_sem,
                device_id={"panel": target})

        def send(t, carry):
            moment_copy(t, early_recv).start()
            return carry

        def send_late(t, carry):
            moment_copy(t, late_recv).start()
            return carry

        def send_down(first, stop):
            @pl.when(chip < last)
            def _():
                lax.fori_loop(first, stop, send, 0)

            @pl.when(chip == last)
            def _():
                lax.fori_loop(first, stop, send_late, 0)

        @pl.when(chip == last)
        def _():
            meet()
            send_late(0, 0)
            send_late(1, 0)
            reply(answer_last)

        @pl.when(chip < last)
        def _():
            lax.fori_loop(0, jnp.minimum(me, 2), send, 0)


        @pl.when(chip >= last - 1)
        def _():
            halo(False).start()

        for k in range(PARTS):
            near_copy(lax.rem(k + (1 - core) * (PARTS // 2), PARTS)).start()
        eval_copy.start()

        @pl.when(has_high)
        def _():
            pl.semaphore_wait(next_ready, 1)
            halo(True).start()

        send_down(2, me)

        def send_up():
            @pl.when(me < count - 3)
            def _():
                pl.semaphore_wait(ready, count - 3 - me)
                lax.fori_loop(me + 1, count - 2, send, 0)

            @pl.when(chip < last)
            def _():
                pl.semaphore_wait(last_ready, 2)
                lax.fori_loop(count - 2, count, send, 0)

            @pl.when(me == count - 2)
            def _():
                pl.semaphore_wait(last_ready, 1)
                send_late(count - 1, 0)

        @pl.when(chip > 0)
        def _():
            send_up()

        neigh_copy.wait()
        live_copy.wait()
        high_copy.wait()
        half = PARTS // 2

        def near_half(field, first, base):
            def near_part(i, carry):
                near_copy(first + i).wait()
                for t in range(part):
                    b = (first + i) * part + t
                    alive = live[b]
                    places = [jnp.clip(neigh[j, b] - base, 0, zero_slot - 1) for j in range(slots)]
                    picked = [field[jnp.where(j < alive, places[j], zero_slot)] for j in range(slots)]
                    weights = jnp.concatenate([near[b, j] for j in range(slots)], axis=1)
                    acc[b] = lax.dot_general(jnp.concatenate(picked, axis=1), weights, CONTRACT_LAST,
                                             preferred_element_type=jnp.float32)
                return carry

            lax.fori_loop(0, half, near_part, 0)

        def low_half():
            @pl.when(has_low)
            def _():
                halo(True).wait_recv()

            near_half(low, 0, me * blk_count - reach)

        def high_half():
            @pl.when(has_high)
            def _():
                halo(False).wait_recv()

            near_half(high, half, me * blk_count)

        @pl.when(core == 1)
        def _():
            low_half()

        @pl.when(core == 0)
        def _():
            high_half()

        @pl.when(chip == 0)
        def _():
            send_up()

        @pl.when(core == 1)
        def _():
            high_half()

        @pl.when(core == 0)
        def _():
            low_half()

        coup_copy.wait()
        eval_copy.wait()

        @pl.when(has_high)
        def _():
            halo(True).wait_send()

        @pl.when(has_low)
        def _():
            halo(False).wait_send()

        bytes_of(count - 1, send_sem).wait()

        @pl.when(chip < last)
        def _():
            bytes_of(count - 3, early_recv).wait()

        @pl.when(chip == last)
        def _():
            bytes_of(count - 2, early_recv).wait()

    dma, signal = pltpu.SemaphoreType.DMA, pltpu.SemaphoreType.REGULAR
    pl.run_scoped(gather, dma((7,)), dma((rest_parts,)), dma((PARTS,)), dma((2,)), dma, dma((2,)), dma,
                  signal, signal, signal)

    sums = [jnp.zeros(moments.shape[2:], jnp.float32) for _ in range(coarse_dev)]

    def weights_of(s):
        return [[coup[c, s * coarse_dev + i] for c in range(coarse_dev)] for i in range(coarse_dev)]

    def add(s, factors):
        for i in range(coarse_dev):
            term = moments[s, i].astype(jnp.float32)
            for c in range(coarse_dev):
                sums[c] += factors[i][c] * term

    for s in range(count - 2):
        add(s, weights_of(s))
    late_factors = [weights_of(s) for s in (count - 2, count - 1)]

    @pl.when(chip < last)
    def _():
        bytes_of(2, late_recv).wait()

    @pl.when(chip == last)
    def _():
        bytes_of(1, late_recv).wait()

    add(count - 2, late_factors[0])
    add(count - 1, late_factors[1])
    spread = [total.astype(jnp.bfloat16) for total in sums]
    blank = jnp.zeros_like(spread[0])
    lhs = jnp.concatenate([jnp.concatenate([e, blank], axis=1) for e in spread]
                          + [jnp.concatenate([blank, e], axis=1) for e in spread], axis=0)
    for b0 in range(0, blk_count, 4):
        rhs = jnp.concatenate([jnp.concatenate([evl[b0 + i], evl[b0 + i + 1]], axis=1) for i in (0, 2)], axis=0)
        far = jnp.dot(lhs, rhs, preferred_element_type=jnp.float32)
        for i in range(4):
            b = b0 + i
            own = cmap[b] - me * coarse_dev
            lanes = slice((i % 2) * panels, (i % 2 + 1) * panels)
            first = (i // 2) * coarse_dev * columns
            part_far = far[first:first + columns, lanes]
            for c in range(1, coarse_dev):
                rows = first + c * columns
                part_far = jnp.where(own == c, far[rows:rows + columns, lanes], part_far)
            out[b] = (acc[b] + part_far).astype(jnp.bfloat16)


def shards(count, density, near_blocks, neighbours, counts, coarse_map, restrict, evaluate, coupling):
    blk_count, columns, panels = density.shape
    terms = restrict.shape[1]
    coarse_dev = coupling.shape[0]
    hbm = pl.BlockSpec(memory_space=pl.ANY)
    dma = pltpu.SemaphoreType.DMA
    return pl.pallas_call(
        functools.partial(kernel, count),
        out_shape=pltpu.VMEM(density.shape, jnp.bfloat16),
        in_specs=[hbm] * 8,
        out_specs=pl.BlockSpec(memory_space=pltpu.VMEM),
        scratch_shapes=[
            pltpu.SMEM(neighbours.shape[::-1], jnp.int32),
            pltpu.SMEM(counts.shape, jnp.int32),
            pltpu.SMEM(coarse_map.shape, jnp.int32),
            pltpu.SMEM(coupling.shape, jnp.float32),
            pltpu.VMEM((blk_count + blk_count // 2 + 1, columns, panels), jnp.bfloat16),
            pltpu.VMEM((blk_count + blk_count // 2 + 1, columns, panels), jnp.bfloat16),
            pltpu.VMEM(near_blocks.shape, jnp.bfloat16),
            pltpu.VMEM(restrict.shape, jnp.bfloat16),
            pltpu.VMEM(evaluate.shape, jnp.bfloat16),
            pltpu.VMEM((blk_count, coarse_dev * columns, panels), jnp.bfloat16),
            pltpu.VMEM((coarse_dev * columns, terms), jnp.float32),
            pltpu.VMEM((count, coarse_dev, columns, terms), jnp.bfloat16),
            pltpu.VMEM(density.shape, jnp.float32),
            dma,
        ],
        compiler_params=pltpu.CompilerParams(collective_id=0, has_side_effects=True),
    )(density, near_blocks, neighbours.T, counts, coarse_map, restrict, evaluate, coupling)


def solution(mesh):
    rows = ("grp", "panel")
    placed = (
        P(rows, None, None),
        P(rows, None, None, None),
        P(rows, None),
        P(rows),
        P(rows),
        P(rows, None, None),
        P(rows, None, None),
        P(rows, None),
    )
    return jax.shard_map(
        functools.partial(shards, mesh.shape["panel"]),
        mesh=mesh,
        in_specs=placed,
        out_specs=P(rows, None, None),
        check_vma=False,
    )
```
